32 devices in a mesh: dp: 8 (over z, y), row: 2 (over x), col: 2 (over core).
Axes of the slice: x: 2, y: 2, z: 4, core: 2. Of those that a mesh axis runs over, the one named last changes fastest.
Arguments:
- hidden_in: bfloat16 [8192, 2048], P(('dp', 'row'), 'col'), may hold values from -6 to 6
- cotangent: bfloat16 [8192, 2048], P(('dp', 'row'), 'col'), may hold values from -6 to 6
- segments: int32 [8192], P('dp'), may hold values from 0 to 64, as said below
- positions: int32 [8192], P('dp'), may hold values from 0 to 959, as said below
- attention_norm_gain: float32 [2048], P('col'), may hold values from 0.1 to 1.9
- attention_norm_bias: float32 [2048], P('col'), may hold values from -2 to 2
- qkv_weight: bfloat16 [2048, 3, 2048], P('col', None, 'row')
- qkv_bias: float32 [3, 2048], P(None, ('row', 'col')), may hold values from -3 to 3
- out_weight: bfloat16 [2048, 2048], P('row', 'col'), may hold values from -1.5 to 1.5
- feedforward_norm_gain: float32 [2048], P('col'), may hold values from 0.1 to 1.9
- feedforward_norm_bias: float32 [2048], P('col'), may hold values from -2 to 2
- gate_up_weight: bfloat16 [2048, 2, 5632], P('col', None, 'row'), may hold values from -0.125 to 0.125
- down_weight: bfloat16 [5632, 2048], P('row', 'col'), may hold values from -0.078125 to 0.078125
Outputs:
- output: bfloat16 [8192, 2048], P(('dp', 'row'), 'col')
- grad_input: bfloat16 [8192, 2048], P(('dp', 'row'), 'col')
- grad_qkv_weight: float32 [2048, 3, 2048], P(('col', 'dp'), None, 'row')
- grad_qkv_bias: float32 [3, 2048], P(None, ('row', 'col', 'dp'))
- grad_out_weight: float32 [2048, 2048], P(('row', 'dp'), 'col')
- grad_gate_up_weight: float32 [2048, 2, 5632], P(('col', 'dp'), None, 'row')
- grad_down_weight: float32 [5632, 2048], P(('row', 'dp'), 'col')
- grad_first_gain: float32 [2048], P('col')
- grad_first_bias: float32 [2048], P('col')
- grad_second_gain: float32 [2048], P('col')
- grad_second_bias: float32 [2048], P('col')
The draws below stay inside these ranges and needn't reach their ends.
Inputs may be any that keep to these rules, and one draw needn't show every extreme that they name: `segments`: within each sequence of 1024 tokens the document numbers start at 0, never fall and rise by at most one from token to token; some sequence reaches 64. `positions`: A token's position counts from 0 at its document's first token; the longest document has exactly 960 tokens.
All inputs are finite; a program needn't handle non-finite values.
Results may differ from the reference program's by a relative error of at most 0.015.
Values may be sent and summed in bfloat16 or wider, within the bound.
A program may use at most 256 MiB of HBM per device.

```python
import math
import jax
import jax.numpy as jnp
from jax import lax

D = 2048
H = 32
HD = 64
FF = 5632
SEQ_LEN = 1024
NSEQ = 8
TOKENS = 8192
DOC_MOST = 960


def document_layout(key):
    base_key = jax.random.fold_in(key, 17)
    key_star, key_first, key_flags = jax.random.split(base_key, 3)
    doc_cap = SEQ_LEN // 16
    chosen = jax.random.randint(key_star, (), 0, NSEQ)
    first_len = jax.random.randint(key_first, (NSEQ,), max(SEQ_LEN // 10, 1), DOC_MOST + 1)
    is_chosen = jnp.arange(NSEQ) == chosen
    first_len = jnp.where(is_chosen, DOC_MOST, first_len)
    start_flags = jax.random.randint(key_flags, (NSEQ, SEQ_LEN), 0, max(SEQ_LEN // 4, 2)) == 0
    order = jnp.arange(SEQ_LEN)[None, :]
    after_first = order > first_len[:, None]
    forced = is_chosen[:, None] & (order >= first_len[:, None])
    starts = (order == 0) | (order == first_len[:, None]) | after_first & start_flags | forced
    counted = jnp.cumsum(starts.astype(jnp.int32), axis=1) - 1
    kept = starts & (counted <= doc_cap)
    segment_ids = jnp.cumsum(kept.astype(jnp.int32), axis=1) - 1
    doc_begin = lax.cummax(jnp.where(kept, order, 0), axis=1)
    return (segment_ids.reshape(-1).astype(jnp.int32), (order - doc_begin).reshape(-1).astype(jnp.int32))


def draw_segments(key, part):
    return document_layout(key)[0]


def draw_positions(key, part):
    return document_layout(key)[1]


def draw_qkv_weight(key, part):
    weight_base = jax.random.normal(key, (D, 3, H, HD), jnp.float32) * D ** (-0.5)
    return weight_base.reshape(D, 3, H * HD).astype(jnp.bfloat16)


def level_of(stream_key, extent, cuts, least, top_value):
    level = 1.0
    for dim, blocks in cuts:
        draws = jax.random.uniform(jax.random.fold_in(jax.random.fold_in(stream_key, 6), dim), (blocks,), jnp.float32, least / len(cuts), top_value / len(cuts))
        level = level * jnp.repeat(jnp.exp(draws), extent[dim] // blocks).reshape((-1,) + (1,) * (len(extent) - 1 - dim))
    return level


def centred(stream_key, dims, deviation, limit, cuts=(), dtype=jnp.bfloat16):
    values = jax.random.normal(stream_key, dims, jnp.float32) * deviation
    if len(cuts) > 0:
        values = level_of(stream_key, dims, cuts, -0.22, 0.18) * values
    return jnp.clip(values, min=-limit, max=limit).astype(dtype)


def setup_inputs(seed: int = 0) -> dict:
    key_of = jax.random.split(jax.random.key(seed), 14)
    hidden_in = centred(key_of[0], (TOKENS, D), 1.0, 6.0, ((0, 16), (1, 2)))
    cotangent = centred(key_of[1], (TOKENS, D), 1.0, 6.0, ((0, 16), (1, 2)))
    segments = draw_segments(jax.random.fold_in(key_of[13], 71), 0)
    positions = draw_positions(jax.random.fold_in(key_of[13], 71), 0)
    attention_norm_gain = jnp.clip(1.0 + 0.18 * jax.random.normal(key_of[4], (D,), jnp.float32), 0.1, 1.9)
    attention_norm_bias = centred(key_of[5], (D,), 0.3, 2.0, ((0, 2),), jnp.float32)
    qkv_weight = draw_qkv_weight(jax.random.fold_in(key_of[13], 71), 0)
    qkv_bias = centred(key_of[7], (3, H * HD), 0.5, 3.0, ((1, 4),), jnp.float32)
    out_weight = centred(key_of[8], (H * HD, D), 16 ** -0.5, 1.5, ((0, 2), (1, 2)))
    feedforward_norm_gain = jnp.clip(1.0 + 0.18 * jax.random.normal(key_of[9], (D,), jnp.float32), 0.1, 1.9)
    feedforward_norm_bias = centred(key_of[10], (D,), 0.3, 2.0, ((0, 2),), jnp.float32)
    gate_up_weight = centred(key_of[11], (D, 2, FF), D ** -0.5, 0.125, ((0, 2), (2, 2)))
    down_weight = centred(key_of[12], (FF, D), FF ** -0.5, 0.078125, ((0, 2), (1, 2)))
    return dict(hidden_in=hidden_in, cotangent=cotangent, segments=segments, positions=positions, attention_norm_gain=attention_norm_gain, attention_norm_bias=attention_norm_bias, qkv_weight=qkv_weight, qkv_bias=qkv_bias, out_weight=out_weight, feedforward_norm_gain=feedforward_norm_gain, feedforward_norm_bias=feedforward_norm_bias, gate_up_weight=gate_up_weight, down_weight=down_weight)


EPS = 1e-05
ROPE_BASE = 10000.0
NEG_FILL = -1e+30

def round_half(values):
    return lax.optimization_barrier(values.astype(jnp.bfloat16)).astype(jnp.float32)

def apply_layer_norm(values, gain, shift):
    mean_row = lax.optimization_barrier(jnp.mean(values, axis=-1, keepdims=True))
    centered = values - mean_row
    variance = lax.optimization_barrier(jnp.mean(centered * centered, axis=-1, keepdims=True))
    inv_std = lax.rsqrt(variance + EPS)
    normed = centered * inv_std
    return (normed * gain[None, :] + shift[None, :], normed, inv_std)

def layer_norm_backward(grad_norm, normed, inv_std, gain):
    scaled = grad_norm * gain[None, :]
    first_mean = lax.optimization_barrier(jnp.mean(scaled, axis=-1, keepdims=True))
    second_mean = lax.optimization_barrier(jnp.mean(scaled * normed, axis=-1, keepdims=True))
    return inv_std * (scaled - first_mean - normed * second_mean)

def rope_tables(positions):
    rot_dims = HD // 4
    half_dims = rot_dims // 2
    exponent = jnp.arange(half_dims).astype(jnp.float32) * (2.0 / rot_dims)
    freq = jnp.exp(-exponent * math.log(ROPE_BASE))
    angle = positions.astype(jnp.float32)[:, None] * freq[None, :]
    return (jnp.cos(angle), jnp.sin(angle))

def rotate(values, cosine, sine, sign):
    rot_dims = values.shape[-1] // 4
    half_dims = rot_dims // 2
    first_part = values[..., :half_dims]
    second_part = values[..., half_dims:rot_dims]
    rest_part = values[..., rot_dims:]
    cos_b = cosine[:, None, :]
    sin_b = sign * sine[:, None, :]
    return jnp.concatenate([first_part * cos_b - second_part * sin_b, second_part * cos_b + first_part * sin_b, rest_part], axis=-1)

def reference(hidden_in, cotangent, segments, positions, attention_norm_gain, attention_norm_bias, qkv_weight, qkv_bias, out_weight, feedforward_norm_gain, feedforward_norm_bias, gate_up_weight, down_weight):
    qkv_w = qkv_weight.astype(jnp.float32)
    out_w = out_weight.astype(jnp.float32)
    gu_w = gate_up_weight.astype(jnp.float32)
    down_w = down_weight.astype(jnp.float32)
    seq_count = hidden_in.shape[0] // SEQ_LEN

    def sequence_step(carried, inputs):
        acc_qkv, acc_bias, acc_out, acc_gu, acc_down, acc_ga, acc_ba, acc_gb, acc_bb = carried
        tokens_in, grad_y, segment_ids, position_ids = inputs
        residual_stream = tokens_in.astype(jnp.float32)
        normalized_first, standardized_first, inverse_deviation_first = apply_layer_norm(residual_stream, attention_norm_gain, attention_norm_bias)
        act_one = round_half(normalized_first)
        qkv_all = jnp.einsum('td,dkf->tkf', act_one, qkv_w) + qkv_bias[None]
        qkv_all = qkv_all.reshape(SEQ_LEN, 3, H, HD)
        cosine, sine = rope_tables(position_ids)
        query = round_half(rotate(qkv_all[:, 0], cosine, sine, 1.0) * 0.125)
        keys_rot = round_half(rotate(qkv_all[:, 1], cosine, sine, 1.0))
        values_raw = round_half(qkv_all[:, 2])
        order = jnp.arange(SEQ_LEN)
        allowed = (segment_ids[:, None] == segment_ids[None, :]) & (order[:, None] >= order[None, :])
        scores = jnp.einsum('qhd,khd->hqk', query, keys_rot)
        scores = jnp.where(allowed[None], scores, NEG_FILL)
        row_max = lax.optimization_barrier(jnp.max(scores, axis=-1, keepdims=True))
        log_total = row_max + jnp.log(lax.optimization_barrier(jnp.sum(jnp.exp(scores - row_max), axis=-1, keepdims=True)))
        probs = jnp.exp(scores - log_total)
        probs_b = round_half(probs)
        attended = round_half(jnp.einsum('hqk,khd->qhd', probs_b, values_raw))
        attended_flat = attended.reshape(SEQ_LEN, H * HD)
        middle_state = residual_stream + jnp.einsum('ta,ad->td', attended_flat, out_w)
        normalized_second, standardized_second, inverse_deviation_second = apply_layer_norm(middle_state, feedforward_norm_gain, feedforward_norm_bias)
        act_two = round_half(normalized_second)
        gate_up = jnp.einsum('td,dkf->tkf', act_two, gu_w)
        gate = gate_up[:, 0]
        up_value = gate_up[:, 1]
        sigmoid_gate = jax.nn.sigmoid(gate)
        mixed = round_half(gate * sigmoid_gate * up_value)
        output = (middle_state + jnp.einsum('tf,fd->td', mixed, down_w)).astype(jnp.bfloat16)
        gradient_layer_output = grad_y.astype(jnp.float32)
        grad_down = jnp.einsum('tf,td->fd', mixed, gradient_layer_output)
        grad_mixed = jnp.einsum('td,fd->tf', gradient_layer_output, down_w)
        grad_gate = grad_mixed * up_value * sigmoid_gate * (1.0 + gate * (1.0 - sigmoid_gate))
        grad_up = grad_mixed * gate * sigmoid_gate
        grad_gu = round_half(jnp.stack([grad_gate, grad_up], axis=1))
        grad_gu_w = jnp.einsum('td,tkf->dkf', act_two, grad_gu)
        gradient_activation_second = jnp.einsum('tkf,dkf->td', grad_gu, gu_w)
        gradient_bias_first = lax.optimization_barrier(jnp.sum(gradient_activation_second * standardized_second, axis=0))
        grad_bb = lax.optimization_barrier(jnp.sum(gradient_activation_second, axis=0))
        gradient_middle_state = gradient_layer_output + layer_norm_backward(gradient_activation_second, standardized_second, inverse_deviation_second, feedforward_norm_gain)
        grad_mid_b = round_half(gradient_middle_state)
        grad_out_w = jnp.einsum('ta,td->ad', attended_flat, grad_mid_b)
        grad_attended = round_half(jnp.einsum('td,ad->ta', grad_mid_b, out_w)).reshape(SEQ_LEN, H, HD)
        delta = lax.optimization_barrier(jnp.sum(grad_attended * attended, axis=-1))
        grad_value = jnp.einsum('hqk,qhd->khd', probs_b, grad_attended)
        grad_probs = jnp.einsum('qhd,khd->hqk', grad_attended, values_raw)
        grad_scores = round_half(probs * (grad_probs - jnp.transpose(delta)[:, :, None]))
        grad_query = jnp.einsum('hqk,khd->qhd', grad_scores, keys_rot)
        grad_key = jnp.einsum('hqk,qhd->khd', grad_scores, query)
        grad_query = rotate(grad_query * 0.125, cosine, sine, -1.0)
        grad_key = rotate(grad_key, cosine, sine, -1.0)
        grad_qkv = jnp.stack([grad_query, grad_key, grad_value], axis=1).reshape(SEQ_LEN, 3, H * HD)
        grad_bias = lax.optimization_barrier(jnp.sum(grad_qkv, axis=0))
        grad_qkv_b = round_half(grad_qkv)
        grad_qkv_w = jnp.einsum('td,tkf->dkf', act_one, grad_qkv_b)
        gradient_activation_first = jnp.einsum('tkf,dkf->td', grad_qkv_b, qkv_w)
        gradient_gain_first = lax.optimization_barrier(jnp.sum(gradient_activation_first * standardized_first, axis=0))
        grad_ba = lax.optimization_barrier(jnp.sum(gradient_activation_first, axis=0))
        gradient_layer_input = (gradient_middle_state + layer_norm_backward(gradient_activation_first, standardized_first, inverse_deviation_first, attention_norm_gain)).astype(jnp.bfloat16)
        carried = (acc_qkv + grad_qkv_w, acc_bias + grad_bias, acc_out + grad_out_w, acc_gu + grad_gu_w, acc_down + grad_down, acc_ga + gradient_gain_first, acc_ba + grad_ba, acc_gb + gradient_bias_first, acc_bb + grad_bb)
        return (carried, (output, gradient_layer_input))
    init = (jnp.zeros((D, 3, H * HD), jnp.float32), jnp.zeros((3, H * HD), jnp.float32), jnp.zeros((H * HD, D), jnp.float32), jnp.zeros((D, 2, FF), jnp.float32), jnp.zeros((FF, D), jnp.float32), jnp.zeros((D,), jnp.float32), jnp.zeros((D,), jnp.float32), jnp.zeros((D,), jnp.float32), jnp.zeros((D,), jnp.float32))
    inputs = (hidden_in.reshape(seq_count, SEQ_LEN, D), cotangent.reshape(seq_count, SEQ_LEN, D), segments.reshape(seq_count, SEQ_LEN), positions.reshape(seq_count, SEQ_LEN))
    sums, stacked = lax.scan(sequence_step, init, inputs)
    output = stacked[0].reshape(seq_count * SEQ_LEN, D)
    grad_input = stacked[1].reshape(seq_count * SEQ_LEN, D)
    return (output, grad_input, sums[0], sums[1], sums[2], sums[3], sums[4], sums[5], sums[6], sums[7], sums[8])
```

```python
import math

import jax
import jax.numpy as jnp
from jax import lax
from jax.experimental import pallas as pl
from jax.experimental.pallas import tpu as pltpu
from jax.sharding import PartitionSpec as P

SEQ_LEN = 1024
EPS = 1e-05
ROPE_BASE = 10000.0
HD=64
NEG=-1e30
BQ=256
NT=(((1,),(1,)),((),()))
NN=(((1,),(0,)),((),()))
TN=(((0,),(0,)),((),()))
f32=jnp.float32; bf16=jnp.bfloat16

def attn_fwd_kernel(r_ref, qo, qt, ko, kt, vo, vt, bias, cos, s1, s2, segq, segk, q_out, k_out, v_out, att, lse, att_s):
    th=qo.shape[0]; seq=2*th
    own=pl.ds(pl.multiple_of(r_ref[0]*th, th), th); oth=pl.ds(pl.multiple_of((1-r_ref[0])*th, th), th)
    def rot(x, where_):
        return x*cos[where_,:]+pltpu.roll(x,120,1)*s1[where_,:]+pltpu.roll(x,8,1)*s2[where_,:]
    for src, where_ in ((0,own),(1,oth)):
        q=(qo,qt)[src][...].astype(f32)+bias[0]
        k=(ko,kt)[src][...].astype(f32)+bias[1]
        v=(vo,vt)[src][...].astype(f32)+bias[2]
        q_out[where_,:]=(rot(q,where_)*0.125).astype(bf16)
        k_out[where_,:]=rot(k,where_).astype(bf16)
        v_out[where_,:]=v.astype(bf16)
    lane=lax.broadcasted_iota(jnp.int32,(1,128),1)
    first=lane<HD
    tri=lax.broadcasted_iota(jnp.int32,(BQ,BQ),0)<=lax.broadcasted_iota(jnp.int32,(BQ,BQ),1)
    for i in range(seq//BQ):
        n=(i+1)*BQ
        rows=pl.ds(i*BQ,BQ)
        q=q_out[rows,:]
        k=k_out[pl.ds(0,n),:]; v=v_out[pl.ds(0,n),:]
        same=segk[pl.ds(0,n),:]==segq[:,rows]
        ps=[];vs=[]
        for h in range(2):
            mk=first if h==0 else ~first
            qh=jnp.where(mk,q,jnp.zeros_like(q))
            s=lax.dot_general(k,qh,NT,preferred_element_type=f32)
            s=jnp.where(same,s,NEG)
            d=jnp.where(tri,s[n-BQ:,:],NEG)
            s=jnp.concatenate([s[:n-BQ,:],d],0) if n>BQ else d
            m=jnp.max(s,axis=0,keepdims=True)
            p=jnp.exp(s-m)
            l=jnp.sum(p,axis=0,keepdims=True)
            lse[0,h:h+1,i*BQ:(i+1)*BQ]=m+jnp.log(l)
            ps.append((p*(1.0/l)).astype(bf16)); vs.append(jnp.where(mk,v,jnp.zeros_like(v)))
        o=lax.dot_general(ps[0],vs[0],TN,preferred_element_type=f32)+lax.dot_general(ps[1],vs[1],TN,preferred_element_type=f32)
        att_s[rows,:]=o.astype(bf16)
    att[pl.ds(0,th),:]=att_s[own,:]
    att[pl.ds(th,th),:]=att_s[oth,:]

def attn_fwd(r, qkv_own, qkv_oth, bias, cos, s1, s2, seg):
    th, w3=qkv_own.shape; w=w3//3; npair=w//128; seq=2*th
    blk=lambda off: pl.BlockSpec((th,128),lambda p,r: (0,off*npair+p))
    full=lambda shape: pl.BlockSpec(shape,lambda p,r: (0,)*len(shape))
    outb=pl.BlockSpec((seq,128),lambda p,r:(0,p))
    return pl.pallas_call(
        attn_fwd_kernel,
        out_shape=[jax.ShapeDtypeStruct((seq,w),bf16)]*4+[jax.ShapeDtypeStruct((npair,8,seq),f32)],
        grid_spec=pltpu.PrefetchScalarGridSpec(num_scalar_prefetch=1,grid=(npair,),
            in_specs=[blk(0),blk(0),blk(1),blk(1),blk(2),blk(2),
              pl.BlockSpec((3,1,128),lambda p,r:(0,0,p)),full((seq,128)),full((seq,128)),full((seq,128)),full((1,seq)),full((seq,1))],
            out_specs=[outb]*4+[pl.BlockSpec((1,8,seq),lambda p,r:(p,0,0))],
            scratch_shapes=[pltpu.VMEM((seq,128),bf16)]),
        compiler_params=pltpu.CompilerParams(vmem_limit_bytes=48<<20),
        name="attention_forward",
        cost_estimate=pl.CostEstimate(flops=4*seq*seq*w,bytes_accessed=seq*w*4*6,transcendentals=seq*seq*w//128),
    )(r, qkv_own,qkv_oth,qkv_own,qkv_oth,qkv_own,qkv_oth,bias.reshape(3,1,w),cos,s1,s2,seg.reshape(1,seq),seg.reshape(seq,1))

def attn_bwd_kernel(r_ref, q_ref, k_ref, v_ref, att, go, gt, lse, cos, s1, s2, segq, segk, dqkv, dbias, dk_acc, dv_acc, dq_s, do_s, att_s):
    th=go.shape[0]; seq=2*th; w=dqkv.shape[1]//3
    p=pl.program_id(0)
    own=pl.ds(pl.multiple_of(r_ref[0]*th, th), th); oth=pl.ds(pl.multiple_of((1-r_ref[0])*th, th), th)
    do_s[own,:]=go[...]; do_s[oth,:]=gt[...]
    att_s[own,:]=att[pl.ds(0,th),:]; att_s[oth,:]=att[pl.ds(th,th),:]
    lane=lax.broadcasted_iota(jnp.int32,(1,128),1)
    first=lane<HD
    sel=jnp.where(lax.broadcasted_iota(jnp.int32,(8,128),0)==0, (lax.broadcasted_iota(jnp.int32,(8,128),1)<HD).astype(f32), (lax.broadcasted_iota(jnp.int32,(8,128),1)>=HD).astype(f32))
    tri=lax.broadcasted_iota(jnp.int32,(BQ,BQ),0)<=lax.broadcasted_iota(jnp.int32,(BQ,BQ),1)
    dk_acc[...]=jnp.zeros_like(dk_acc); dv_acc[...]=jnp.zeros_like(dv_acc)
    for i in range(seq//BQ):
        n=(i+1)*BQ
        rows=pl.ds(i*BQ,BQ)
        q=q_ref[rows,:]; do=do_s[rows,:]
        k=k_ref[pl.ds(0,n),:]; v=v_ref[pl.ds(0,n),:]
        prod=do.astype(f32)*att_s[rows,:].astype(f32)
        delta=lax.dot_general(sel,prod,NT,preferred_element_type=f32,precision=lax.Precision.HIGHEST)
        same=segk[pl.ds(0,n),:]==segq[:,rows]
        ps=[];dss=[];dos=[];qs=[];ks=[]
        for h in range(2):
            mk=first if h==0 else ~first
            qh=jnp.where(mk,q,jnp.zeros_like(q)); doh=jnp.where(mk,do,jnp.zeros_like(do)); kh=jnp.where(mk,k,jnp.zeros_like(k))
            s=lax.dot_general(k,qh,NT,preferred_element_type=f32)
            s=jnp.where(same,s,NEG)
            d=jnp.where(tri,s[n-BQ:,:],NEG)
            s=jnp.concatenate([s[:n-BQ,:],d],0) if n>BQ else d
            pt=jnp.exp(s-lse[0,h:h+1,i*BQ:(i+1)*BQ])
            dp=lax.dot_general(v,doh,NT,preferred_element_type=f32)
            ds=(pt*(dp-delta[h:h+1,:])).astype(bf16)
            ps.append(pt.astype(bf16)); dss.append(ds); dos.append(doh); qs.append(qh); ks.append(kh)
        dv_acc[pl.ds(0,n),:]+=lax.dot_general(jnp.concatenate(ps,1),jnp.concatenate(dos,0),NN,preferred_element_type=f32)
        dk_acc[pl.ds(0,n),:]+=lax.dot_general(jnp.concatenate(dss,1),jnp.concatenate(qs,0),NN,preferred_element_type=f32)
        dq_s[rows,:]=lax.dot_general(dss[0],ks[0],TN,preferred_element_type=f32)+lax.dot_general(dss[1],ks[1],TN,preferred_element_type=f32)
    def back(x):
        return x*cos[...]-pltpu.roll(x,120,1)*s1[...]-pltpu.roll(x,8,1)*s2[...]
    dq_s[...]=back(dq_s[...]*0.125)
    dk_acc[...]=back(dk_acc[...])
    for j,ref in enumerate((dq_s,dk_acc,dv_acc)):
        cols=pl.ds(pl.multiple_of(j*w+p*128,128),128)
        dqkv[pl.ds(0,th),cols]=ref[own,:].astype(bf16)
        dqkv[pl.ds(th,th),cols]=ref[oth,:].astype(bf16)
        dbias[0,j:j+1,:]=jnp.sum(ref[...],axis=0,keepdims=True)

def attn_bwd(r, q,k,v,att,g_own,g_oth,lse,cos,s1,s2,seg):
    seq,w=q.shape; npair=w//128; th=seq//2
    full=lambda shape: pl.BlockSpec(shape,lambda p,r: (0,)*len(shape))
    b=pl.BlockSpec((seq,128),lambda p,r:(0,p)); hb=pl.BlockSpec((th,128),lambda p,r:(0,p))
    return pl.pallas_call(
        attn_bwd_kernel,
        out_shape=[jax.ShapeDtypeStruct((seq,3*w),bf16),jax.ShapeDtypeStruct((npair,8,128),f32)],
        grid_spec=pltpu.PrefetchScalarGridSpec(num_scalar_prefetch=1,grid=(npair,),
            in_specs=[b,b,b,b,hb,hb,pl.BlockSpec((1,8,seq),lambda p,r:(p,0,0)),full((seq,128)),full((seq,128)),full((seq,128)),full((1,seq)),full((seq,1))],
            out_specs=[full((seq,3*w)),pl.BlockSpec((1,8,128),lambda p,r:(p,0,0))],
            scratch_shapes=[pltpu.VMEM((seq,128),f32)]*3+[pltpu.VMEM((seq,128),bf16)]*2),
        compiler_params=pltpu.CompilerParams(vmem_limit_bytes=56<<20),
        name="attention_backward",
        cost_estimate=pl.CostEstimate(flops=10*seq*seq*w,bytes_accessed=seq*w*2*9,transcendentals=seq*seq*w//128),
    )(r,q,k,v,att,g_own,g_oth,lse,cos,s1,s2,seg.reshape(1,seq),seg.reshape(seq,1))

def tables(positions):
    lane=jnp.arange(128)%HD
    half=HD//8
    freq=jnp.where(lane<2*half, jnp.exp(-((lane%half).astype(f32)*(2.0/(2*half)))*math.log(ROPE_BASE)), 0.0)
    ang=positions.astype(f32)[:,None]*freq[None,:]
    c=jnp.cos(ang); s=jnp.sin(ang)
    return c, jnp.where(lane<half,-s,0.0), jnp.where((lane>=half)&(lane<2*half),s,0.0)


def pairs(count, step=1):
    return [(i, i ^ step) for i in range(count)]


def swap(values, axis):
    return lax.ppermute(values, axis, pairs(2))


def after(values, *others):
    return lax.optimization_barrier((values,) + others)[0]


def row_slice(values, index, count):
    return lax.dynamic_slice_in_dim(values, index * count, count, 0)


def mm(a, b, dims=NN):
    return lax.dot_general(a, b, dims, preferred_element_type=f32)


def joined(first_half, second_half):
    return jnp.concatenate([first_half, second_half], axis=1)


def stacked(first_half, second_half):
    return jnp.concatenate([first_half, second_half], axis=0)


def moments(values, width):
    mean = jnp.sum(values, axis=1, keepdims=True) / width
    centered = values - mean
    inv = lax.rsqrt(jnp.sum(centered * centered, axis=1, keepdims=True) / width + EPS)
    return mean, inv


def make_body(dp_count):
    bit_count = dp_count.bit_length() - 1
    assert 1 << bit_count == dp_count

    def body(
        hidden_in,
        cotangent,
        segments,
        positions,
        attention_norm_gain,
        attention_norm_bias,
        qkv_weight,
        qkv_bias,
        out_weight,
        feedforward_norm_gain,
        feedforward_norm_bias,
        gate_up_weight,
        down_weight,
    ):
        th, dl = hidden_in.shape
        assert segments.shape[0] == 2 * th == SEQ_LEN
        width = 2 * dl
        fq = qkv_bias.shape[1]
        ff = down_weight.shape[0] // 2
        c = lax.axis_index("col")
        r = lax.axis_index("row")
        dp = lax.axis_index("dp")
        bits = [(dp >> b) & 1 for b in range(bit_count)]
        r_arr = jnp.reshape(r, (1,)).astype(jnp.int32)

        def phase(block, axis, bit):
            send = lax.dynamic_index_in_dim(block, 1 - bits[bit], axis, keepdims=False)
            got = lax.ppermute(send, "dp", pairs(dp_count, 1 << bit))
            keep = lax.dynamic_index_in_dim(block, bits[bit], axis, keepdims=False)
            return (keep.astype(f32) + got.astype(f32)).astype(bf16)

        def reduce_bits(block, order, top):
            rows, cols = block.shape
            left = list(range(top - 1, -1, -1))
            block = block.reshape((2,) * top + (rows >> top, cols))
            for bit in order:
                block = phase(block, left.index(bit), bit)
                left.remove(bit)
            return block

        def top_phase(own, par):
            mine = bits[-1] == c
            send = jnp.where(mine, par, own)
            got = lax.ppermute(send, "dp", pairs(dp_count, dp_count >> 1))
            keep = jnp.where(mine, own, par)
            return keep.astype(f32) + got.astype(f32)

        h_x = swap(hidden_in, "row")
        h_c = swap(hidden_in, "col")
        norms = jnp.stack(
            [
                attention_norm_gain,
                attention_norm_bias,
                feedforward_norm_gain,
                feedforward_norm_bias,
            ]
        )
        norms_c = swap(norms, "col")
        q_part = lambda i: lax.dynamic_slice_in_dim(qkv_weight, i * fq, fq, 2).reshape(dl, 3 * fq)
        w_qkv = stacked(q_part(c), swap(q_part(1 - c), "col"))
        wo_own = row_slice(out_weight, c, fq)
        wo_par = row_slice(out_weight, 1 - c, fq)
        wo_t = joined(wo_own, swap(wo_par, "col"))
        g_part = lambda i: lax.dynamic_slice_in_dim(gate_up_weight, i * ff, ff, 2).reshape(
            dl, 2 * ff
        )
        w_gu = stacked(g_part(c), swap(g_part(1 - c), "col"))
        wd_own = row_slice(down_weight, c, ff)
        wd_par = row_slice(down_weight, 1 - c, ff)
        wd_t = joined(wd_own, swap(wd_par, "col"))
        h_xc = swap(h_x, "col")
        cot_x = swap(after(cotangent, h_x), "row")
        cot_c = swap(cotangent, "col")
        cot_xc = swap(cot_x, "col")
        cos, s1, s2 = tables(positions)

        def norm_one(low, high):
            full = joined(low, high).astype(f32)
            mean, inv = moments(full, width)
            gain = jnp.concatenate([norms[0], norms_c[0]])
            bias = jnp.concatenate([norms[1], norms_c[1]])
            return ((full - mean) * inv * gain + bias).astype(bf16), mean, inv

        act_own, mean_one, inv_one = norm_one(hidden_in, h_c)
        act_oth, _, _ = norm_one(h_x, h_xc)
        qkv_own = mm(act_own, w_qkv)
        qkv_oth = mm(act_oth, w_qkv)
        query, key, value, att, lse = attn_fwd(
            r_arr, qkv_own, qkv_oth, qkv_bias, cos, s1, s2, segments
        )
        att_p = swap(att, "col")
        att_full = joined(att, att_p)
        wo_rel = stacked(wo_own, wo_par)
        part_oth = mm(att_full[th:], wo_rel).astype(bf16)
        part_got = swap(part_oth, "row")
        mid = hidden_in.astype(f32) + mm(att_full[:th], wo_rel) + part_got.astype(f32)

        total = lax.psum(jnp.sum(mid, axis=1), "col")
        mean_two = (total / width)[:, None]
        square = lax.psum(jnp.sum((mid - mean_two) ** 2, axis=1), "col")
        inv_two = lax.rsqrt(square / width + EPS)[:, None]
        xhat_two = (mid - mean_two) * inv_two
        act_two = (xhat_two * norms[2] + norms[3]).astype(bf16)
        a2_x = swap(act_two, "row")
        a2_c = swap(act_two, "col")
        a2_xc = swap(a2_x, "col")
        a2_own = joined(act_two, a2_c)
        a2_oth = joined(a2_x, a2_xc)

        def feed(act, low, high):
            grad_mixed = mm(joined(low, high), wd_t, NT).astype(bf16)
            gate_up = mm(act, w_gu)
            gate = gate_up[:, :ff]
            up = gate_up[:, ff:]
            sig = jax.nn.sigmoid(gate)
            mixed = (gate * sig * up).astype(bf16)
            gm = grad_mixed.astype(f32)
            grad_gate = gm * up * sig * (1.0 + gate * (1.0 - sig))
            grad_up = gm * gate * sig
            return mixed, joined(grad_gate.astype(bf16), grad_up.astype(bf16))

        mixed_own, ggu_own = feed(a2_own, cotangent, cot_c)
        mixed_oth, ggu_oth = feed(a2_oth, cot_x, cot_xc)

        def core_sum(partial_value):
            got = swap(partial_value[:, dl:].astype(bf16), "col")
            return partial_value[:, :dl] + got.astype(f32)

        ga2_oth = core_sum(mm(ggu_oth, w_gu, NT)).astype(bf16)
        ga2_got = swap(ga2_oth, "row")

        mixed = stacked(mixed_own, mixed_oth)
        mixed_p = swap(mixed, "col")
        cot_rows = stacked(cotangent, cot_x)
        order_a = list(range(bit_count - 1))
        order_b = order_a[1:] + order_a[:1]
        gd_own = mm(mixed, cot_rows, TN).astype(bf16)
        gd_par = mm(mixed_p, cot_rows, TN).astype(bf16)
        gd_own = reduce_bits(gd_own, order_a, bit_count - 1)
        gd_par = reduce_bits(gd_par, order_b, bit_count - 1)
        grad_down_w = top_phase(gd_own, gd_par)

        order_a = list(range(bit_count))
        order_b = [order_a[1], order_a[0]] + order_a[2:]
        ggu = stacked(ggu_own, ggu_oth)
        low_acts = stacked(act_two, a2_x)
        high_acts = stacked(a2_c, a2_xc)
        gg_low = reduce_bits(mm(low_acts, ggu, TN).astype(bf16), order_a, bit_count)
        gg_high = reduce_bits(mm(high_acts, ggu, TN).astype(bf16), order_a, bit_count)

        def column_halves(low, high, parts):
            other = swap(high, "col")
            rows = low.shape[0]
            low = low.reshape(rows, parts, -1)
            other = other.reshape(rows, parts, -1)
            first_half = jnp.where(c == 0, low, other)
            second_half = jnp.where(c == 0, other, low)
            return jnp.concatenate([first_half, second_half], axis=2).astype(f32)

        grad_gu_w = column_halves(gg_low, gg_high, 2)

        ga2 = core_sum(mm(ggu_own, w_gu, NT)) + ga2_got.astype(f32)
        sum_gain_two = jnp.sum(ga2 * xhat_two, axis=0)
        sum_bias_two = jnp.sum(ga2, axis=0)

        def norm_backward(grad_norm, xhat, inv, gain):
            scaled = grad_norm * gain
            sums = lax.psum(
                jnp.stack([jnp.sum(scaled, axis=1), jnp.sum(scaled * xhat, axis=1)]), "col"
            )
            return inv * (scaled - (sums[0] / width)[:, None] - xhat * (sums[1] / width)[:, None])

        grad_mid = cotangent.astype(f32) + norm_backward(ga2, xhat_two, inv_two, norms[2])
        gmb = grad_mid.astype(bf16)
        gmb_x = swap(gmb, "row")
        gmb_c = swap(gmb, "col")
        gmb_xc = swap(gmb_x, "col")
        gatt_own = mm(joined(gmb, gmb_c), wo_t, NT).astype(bf16)
        gatt_oth = mm(joined(gmb_x, gmb_xc), wo_t, NT).astype(bf16)

        down_oth = mm(mixed_oth, wd_own) + mm(mixed_p[th:], wd_par)
        down_got = swap(after(down_oth.astype(bf16), gmb_x), "row")
        down_own = mm(mixed_own, wd_own) + mm(mixed_p[:th], wd_par)
        output = (mid + down_own + down_got.astype(f32)).astype(bf16)

        dqkv, dbias = attn_bwd(
            r_arr, query, key, value, att, gatt_own, gatt_oth, lse, cos, s1, s2, segments
        )
        gmb_rows = stacked(gmb, gmb_x)
        go_own = mm(att, gmb_rows, TN).astype(bf16)
        go_par = mm(att_p, gmb_rows, TN).astype(bf16)
        order_o = list(range(bit_count - 1))
        grad_out_w = top_phase(
            reduce_bits(go_own, order_o, bit_count - 1),
            reduce_bits(go_par, order_o, bit_count - 1),
        )

        ga1_oth = core_sum(mm(dqkv[th:], w_qkv, NT)).astype(bf16)
        ga1_got = swap(ga1_oth, "row")
        act_low = stacked(act_own[:, :dl], act_oth[:, :dl])
        act_high = stacked(act_own[:, dl:], act_oth[:, dl:])
        gq_low = reduce_bits(mm(act_low, dqkv, TN).astype(bf16), order_a, bit_count)
        gq_high = reduce_bits(mm(act_high, dqkv, TN).astype(bf16), order_b, bit_count)
        grad_qkv_w = column_halves(gq_low, gq_high, 3)

        ga1 = core_sum(mm(dqkv[:th], w_qkv, NT)) + ga1_got.astype(f32)
        xhat_one = (hidden_in.astype(f32) - mean_one) * inv_one
        grad_input = (grad_mid + norm_backward(ga1, xhat_one, inv_one, norms[0])).astype(bf16)

        sums = jnp.stack(
            [jnp.sum(ga1 * xhat_one, axis=0), jnp.sum(ga1, axis=0), sum_gain_two, sum_bias_two]
        )
        sums = sums + swap(sums, "row")
        bias_sums = jnp.transpose(dbias[:, :3], (1, 0, 2)).reshape(1, 3 * fq)
        flat = jnp.concatenate([sums.reshape(1, 4 * dl), bias_sums], axis=1)
        for b in range(bit_count):
            flat = flat + lax.ppermute(flat, "dp", pairs(dp_count, 1 << b))
        sums = flat[0, : 4 * dl].reshape(4, dl)
        bias_all = flat[0, 4 * dl :].reshape(3, fq)
        piece = fq // dp_count
        grad_qkv_bias = lax.dynamic_slice_in_dim(bias_all, dp * piece, piece, 1)
        return (
            output,
            grad_input,
            grad_qkv_w,
            grad_qkv_bias,
            grad_out_w,
            grad_gu_w,
            grad_down_w,
            sums[0],
            sums[1],
            sums[2],
            sums[3],
        )

    return body


def solution(mesh):
    assert mesh.shape["row"] == 2 and mesh.shape["col"] == 2
    placed = (
        P(("dp", "row"), "col"),
        P(("dp", "row"), "col"),
        P("dp"),
        P("dp"),
        P("col"),
        P("col"),
        P("col", None, "row"),
        P(None, ("row", "col")),
        P("row", "col"),
        P("col"),
        P("col"),
        P("col", None, "row"),
        P("row", "col"),
    )
    return jax.shard_map(
        make_body(mesh.shape["dp"]),
        mesh=mesh,
        in_specs=placed,
        out_specs=(
            P(("dp", "row"), "col"),
            P(("dp", "row"), "col"),
            P(("col", "dp"), None, "row"),
            P(None, ("row", "col", "dp")),
            P(("row", "dp"), "col"),
            P(("col", "dp"), None, "row"),
            P(("row", "dp"), "col"),
            P("col"),
            P("col"),
            P("col"),
            P("col"),
        ),
        check_vma=False,
    )
```
